32 devices in a mesh: rows: 8 (over y, x, core), model: 4 (over z).
Axes of the slice: x: 2, y: 2, z: 4, core: 2. Of those that a mesh axis runs over, the one named last changes fastest.
Arguments:
- weight_gate: bfloat16 [2048, 8192], P('rows', 'model'), may hold values from -0.125 to 0.125
- low_gate: bfloat16 [2048, 64], P('rows'), may hold values from -0.125 to 0.125
- high_gate: bfloat16 [64, 8192], P(None, 'model'), may hold values from -0.75 to 0.75
- weight_up: bfloat16 [2048, 8192], P('rows', 'model'), may hold values from -0.125 to 0.125
- low_up: bfloat16 [2048, 64], P('rows'), may hold values from -0.125 to 0.125
- high_up: bfloat16 [64, 8192], P(None, 'model'), may hold values from -0.75 to 0.75
- weight_down: bfloat16 [8192, 2048], P('model', 'rows'), may hold values from -0.0625 to 0.0625
- low_down: bfloat16 [8192, 64], P('model'), may hold values from -0.0625 to 0.0625
- high_down: bfloat16 [64, 2048], P(None, 'rows'), may hold values from -0.75 to 0.75
- norm_train: float32 [2048], P(('rows', 'model')), may hold values from 0.25 to 1.75
- norm_step: float32 [2048], P(('rows', 'model')), may hold values from -0.3 to 0.3
Outputs:
- final_gate: bfloat16 [8192, 2048], P('model')
- final_up: bfloat16 [8192, 2048], P('model')
- final_down: bfloat16 [2048, 8192], P(None, 'model')
- serve_norm: bfloat16 [2048], replicated
The draws below stay inside these ranges and needn't reach their ends.
All inputs are finite; a program needn't handle non-finite values.
Results may differ from the reference program's by a relative error of at most 0.001.
Values may be sent and summed in bfloat16 or wider, within the bound.
A program may use at most 192 MiB of HBM per device.

```python
import jax
import jax.numpy as jnp

D_MODEL = 2048
D_INNER = 8192
RANK = 64


def block_scale(own_key, extent, split, least, top_value):
    def one(position, shards_of):
        steps = jax.random.uniform(jax.random.fold_in(jax.random.fold_in(own_key, 6), position), (shards_of,), jnp.float32, least / len(split), top_value / len(split))
        return jnp.repeat(jnp.exp(steps), extent[position] // shards_of).reshape((-1,) + (1,) * (len(extent) - position - 1))

    level = one(*split[0])
    for cut in split[1:]:
        level = level * one(*cut)
    return level


def bell_draw(rng, shape, scale, limit, pieces=(), dtype=jnp.bfloat16):
    drawn = jax.random.normal(rng, shape, jnp.float32) * scale
    if len(pieces) > 0:
        drawn = block_scale(rng, shape, pieces, -0.22, 0.18) * drawn
    return jnp.clip(drawn, min=-limit, max=limit).astype(dtype)


def setup_inputs(seed: int = 0) -> dict:
    keys = jax.random.split(jax.random.key(seed), 12)
    return {
        "weight_gate": bell_draw(keys[0], (D_MODEL, D_INNER), D_MODEL ** -0.5, 0.125, ((0, 8), (1, 4))),
        "low_gate": bell_draw(keys[1], (D_MODEL, RANK), D_MODEL ** -0.5, 0.125, ((0, 8),)),
        "high_gate": bell_draw(keys[2], (RANK, D_INNER), RANK ** -0.5, 0.75, ((1, 4),)),
        "weight_up": bell_draw(keys[3], (D_MODEL, D_INNER), D_MODEL ** -0.5, 0.125, ((0, 8), (1, 4))),
        "low_up": bell_draw(keys[4], (D_MODEL, RANK), D_MODEL ** -0.5, 0.125, ((0, 8),)),
        "high_up": bell_draw(keys[5], (RANK, D_INNER), RANK ** -0.5, 0.75, ((1, 4),)),
        "weight_down": bell_draw(keys[6], (D_INNER, D_MODEL), D_INNER ** -0.5, 0.0625, ((0, 4), (1, 8))),
        "low_down": bell_draw(keys[7], (D_INNER, RANK), D_INNER ** -0.5, 0.0625, ((0, 4),)),
        "high_down": bell_draw(keys[8], (RANK, D_MODEL), RANK ** -0.5, 0.75, ((1, 8),)),
        "norm_train": jnp.clip(1.0 + 0.15 * jax.random.normal(keys[9], (D_MODEL,), jnp.float32), 0.25, 1.75),
        "norm_step": jnp.clip(jax.random.uniform(keys[10], (D_MODEL,), jnp.float32, -0.3, 0.3) * block_scale(keys[10], (D_MODEL,), ((0, 32),), -0.4, 0.0), -0.3, 0.3),
    }


mix_rate = 0.5


def reference(weight_gate, low_gate, high_gate, weight_up, low_up, high_up, weight_down, low_down, high_down, norm_train, norm_step):
    result_gate = weight_gate.astype(jnp.float32) + mix_rate * jnp.dot(low_gate, high_gate, preferred_element_type=jnp.float32)
    result_up = weight_up.astype(jnp.float32) + mix_rate * jnp.dot(low_up, high_up, preferred_element_type=jnp.float32)
    result_down = weight_down.astype(jnp.float32) + mix_rate * jnp.dot(low_down, high_down, preferred_element_type=jnp.float32)
    final_gate = result_gate.T.astype(jnp.bfloat16)
    final_up = result_up.T.astype(jnp.bfloat16)
    final_down = result_down.T.astype(jnp.bfloat16)
    serve_norm = (norm_train + norm_step).astype(jnp.bfloat16)
    return final_gate, final_up, final_down, serve_norm
```

```python
import functools

import jax
import jax.numpy as jnp
from jax import lax
from jax.experimental import pallas as pl
from jax.experimental.pallas import tpu as pltpu
from jax.sharding import PartitionSpec as P

mix_rate = 0.5
MESH = pl.DeviceIdType.MESH
PIECES = 4
SIDE = 2


def gather_kernel(
    rows,
    model,
    *refs,
):
    sources, (og, ou, od, norm), refs = refs[:11], refs[11:15], refs[15:]
    held, refs = refs[:11], refs[11:]
    wg, lg, hg, wu, lu, hu, wd, ld, hd, nt, ns = held
    fetch_sem, link_send, link_recv, pair_send, pair_recv, norm_send, norm_recv = refs
    me = lax.axis_index("rows")
    depth = lax.axis_index("model")
    core = lax.rem(me, 2)
    x = lax.rem(me // 2, SIDE)
    y = me // (2 * SIDE)

    def device(y, x, core):
        return (y * SIDE + x) * 2 + core

    pair = device(y, x, 1 - core)
    near_x = device(y, 1 - x, core)
    near_y = device(1 - y, x, core)
    far = device(1 - y, 1 - x, core)

    def shifted(position, size, step):
        return lax.rem(position + step, size)

    barrier = pltpu.get_barrier_semaphore()
    for step in range(1, rows):
        pl.semaphore_signal(barrier, inc=1, device_id={"rows": shifted(me, rows, step)}, device_id_type=MESH)
    for step in range(1, model):
        pl.semaphore_signal(barrier, inc=1, device_id={"model": shifted(depth, model, step)}, device_id_type=MESH)

    outs = (og, ou, od)
    fetches = {}

    def fetch(key, i, *cut):
        fetches[key] = pltpu.make_async_copy(
            sources[i].at[cut] if cut else sources[i], held[i].at[cut] if cut else held[i],
            fetch_sem.at[len(fetches)],
        )

    long = wg.shape[1] // PIECES
    long_down = wd.shape[0] // PIECES
    short = wg.shape[0]
    short_down = wd.shape[1]
    units = [(a, k) for k in range(PIECES) for a in range(3)]

    for u, (a, k) in enumerate(units):
        if k == 0:
            fetch(("low", a), 3 * a + 1)
            fetch(("high", a), 3 * a + 2)
        if a < 2:
            fetch(u, 3 * a, pl.ds(0, short), pl.ds(k * long, long))
        else:
            fetch(u, 3 * a, pl.ds(k * long_down, long_down), pl.ds(0, short_down))
    fetch("train", 9)
    fetch("step", 10)
    for f in fetches.values():
        f.start()

    def place(u, owner):
        a, k = units[u]
        if a < 2:
            return outs[a].at[pl.ds(k * long, long), pl.ds(pl.multiple_of(owner * short, short), short)]
        return outs[a].at[pl.ds(pl.multiple_of(owner * short_down, short_down), short_down), pl.ds(k * long_down, long_down)]

    def compute(u):
        a, k = units[u]
        if k == 0:
            fetches["low", a].wait()
            fetches["high", a].wait()
        fetches[u].wait()
        if a < 2:
            w, low, high = ((wg, lg, hg), (wu, lu, hu))[a]
            cut = slice(k * long, (k + 1) * long)
            weight, low, high = w[:, cut], low[...], high[:, cut]
        else:
            cut = slice(k * long_down, (k + 1) * long_down)
            weight, low, high = wd[cut, :], ld[:, cut], hd[...]
        merged = weight.astype(jnp.float32) + mix_rate * lax.dot_general(
            low, high, (((0,), (0,)), ((), ())), preferred_element_type=jnp.float32
        )
        place(u, me)[...] = merged.astype(jnp.bfloat16).T

    def copy(u, owner, send, recv, target):
        return pltpu.make_async_remote_copy(
            src_ref=place(u, owner), dst_ref=place(u, owner), send_sem=send, recv_sem=recv,
            device_id={"rows": target}, device_id_type=MESH,
        )

    def link(lane, u, owner, target):
        return copy(u, owner, link_send.at[lane, u], link_recv.at[lane, u], target)

    def across(lane, u, owner):
        return copy(u, owner, pair_send.at[lane, u], pair_recv.at[lane, u], pair)

    def send_own(u):
        link(0, u, me, near_x).start()
        link(1, u, me, near_y).start()
        across(3, u, me).start()

    count = len(units)
    compute(0)
    fetches["train"].wait()
    fetches["step"].wait()
    norm[me, depth] = jnp.zeros(norm.shape[2:], norm.dtype)
    norm[me, depth, :, : nt.shape[1]] = nt[...] + ns[...]
    pl.semaphore_wait(barrier, rows - 1 + model - 1)
    for u in range(1, count):
        compute(u)
        send_own(u - 1)

    def norm_copy(step, send):
        if step < model:
            to = {"model": shifted(depth, model, step)}
            ref = norm.at[me, depth] if send else norm.at[me, shifted(depth, model, model - step)]
            slot = step - 1
        else:
            step = step - model + 1
            to = {"rows": shifted(me, rows, step)}
            ref = norm.at[me] if send else norm.at[shifted(me, rows, rows - step)]
            slot = model - 1 + step - 1
        return pltpu.make_async_remote_copy(
            src_ref=ref, dst_ref=ref, send_sem=norm_send.at[slot], recv_sem=norm_recv.at[slot],
            device_id=to, device_id_type=MESH,
        )

    for step in range(1, model):
        norm_copy(step, True).start()
    send_own(count - 1)
    for step in range(1, model):
        norm_copy(step, False).wait_recv()
    for step in range(model, model + rows - 1):
        norm_copy(step, True).start()

    for u in range(count):
        link(0, u, near_x, near_x).wait_recv()
        if u % 2 == 0:
            link(2, u, near_x, near_y).start()
        across(0, u, near_x).start()
        link(1, u, near_y, near_y).wait_recv()
        if u % 2 == 1:
            link(2, u, near_y, near_x).start()
        across(1, u, near_y).start()
    for u in range(count):
        link(2, u, far, near_x).wait_recv()
        across(2, u, far).start()

    for step in range(model, model + rows - 1):
        norm_copy(step, False).wait_recv()
    for step in range(1, model + rows - 1):
        norm_copy(step, True).wait_send()
    pair_x, pair_y = device(y, 1 - x, 1 - core), device(1 - y, x, 1 - core)
    pair_far = device(1 - y, 1 - x, 1 - core)
    for u in range(count):
        link(0, u, me, near_x).wait_send()
        link(1, u, me, near_y).wait_send()
        link(2, u, near_x if u % 2 == 0 else near_y, near_x).wait_send()
        for lane, mine, theirs in ((3, me, pair), (0, near_x, pair_x), (1, near_y, pair_y), (2, far, pair_far)):
            across(lane, u, mine).wait_send()
            across(lane, u, theirs).wait_recv()


def gathered(rows, model, arrays):
    weight_gate, weight_up, weight_down, norm_train = arrays[0], arrays[3], arrays[6], arrays[9]
    shapes = [
        (weight_gate.shape[1], weight_gate.shape[0] * rows),
        (weight_up.shape[1], weight_up.shape[0] * rows),
        (weight_down.shape[1] * rows, weight_down.shape[0]),
    ]
    lanes = -(-norm_train.shape[1] // 128) * 128
    count = 3 * PIECES
    small = rows - 1 + model - 1
    dma = pltpu.SemaphoreType.DMA
    vmem = pl.BlockSpec(memory_space=pltpu.VMEM)
    return pl.pallas_call(
        functools.partial(gather_kernel, rows, model),
        out_shape=[pltpu.VMEM(s, jnp.bfloat16) for s in shapes] + [pltpu.VMEM((rows, model, 1, lanes), jnp.float32)],
        in_specs=[pl.BlockSpec(memory_space=pltpu.HBM)] * len(arrays),
        out_specs=[vmem] * 4,
        scratch_shapes=[pltpu.VMEM(a.shape, a.dtype) for a in arrays]
        + [
            dma((count + 8,)),
            dma((3, count)), dma((3, count)), dma((4, count)), dma((4, count)), dma((small,)), dma((small,)),
        ],
        compiler_params=pltpu.CompilerParams(collective_id=0, has_side_effects=True, vmem_limit_bytes=39 * 2**20 + 5 * 2**17),
    )(*arrays)


def write_kernel(g, u, d, og, ou, od, sems):
    copies = [pltpu.make_async_copy(s, t, sems.at[i]) for i, (s, t) in enumerate(((g, og), (u, ou), (d, od)))]
    for c in copies:
        c.start()
    for c in copies:
        c.wait()


def written(arrays):
    return pl.pallas_call(
        write_kernel,
        out_shape=[jax.ShapeDtypeStruct(a.shape, a.dtype) for a in arrays],
        in_specs=[pl.BlockSpec(memory_space=pltpu.VMEM)] * 3,
        out_specs=[pl.BlockSpec(memory_space=pltpu.HBM)] * 3,
        scratch_shapes=[pltpu.SemaphoreType.DMA((3,))],
        compiler_params=pltpu.CompilerParams(vmem_limit_bytes=2**20),
    )(*arrays)


def local_kernel(rows, model, *arrays):
    arrays = tuple(a.T if i in (1, 4, 7) else a for i, a in enumerate(arrays[:9])) + tuple(
        a.reshape(1, -1) for a in arrays[9:]
    )
    gate, up, down, norm = gathered(rows, model, arrays)
    norm_size = arrays[9].shape[1]
    serve_norm = norm[:, :, 0, :norm_size].astype(jnp.bfloat16).reshape(-1)
    gate, up, down = written((gate, up, down))
    return gate, up, down, serve_norm


def merge(weight, low, high):
    full = weight.astype(jnp.float32) + mix_rate * jnp.dot(low, high, preferred_element_type=jnp.float32)
    return full.astype(jnp.bfloat16).T


def local_plain(*arrays):
    gate, up, down = merge(*arrays[:3]), merge(*arrays[3:6]), merge(*arrays[6:9])
    return (
        lax.all_gather(gate, "rows", axis=1, tiled=True),
        lax.all_gather(up, "rows", axis=1, tiled=True),
        lax.all_gather(down, "rows", axis=0, tiled=True),
        lax.all_gather((arrays[9] + arrays[10]).astype(jnp.bfloat16), ("rows", "model"), axis=0, tiled=True),
    )


def solution(mesh):
    rows, model = mesh.shape["rows"], mesh.shape["model"]
    local = functools.partial(local_kernel, rows, model) if rows == 2 * SIDE * SIDE else local_plain
    in_specs = (
        P("rows", "model"), P("rows", None), P(None, "model"),
        P("rows", "model"), P("rows", None), P(None, "model"),
        P("model", "rows"), P("model", None), P(None, "rows"),
        P(("rows", "model")), P(("rows", "model")),
    )
    out_specs = (P("model", None), P("model", None), P(None, "model"), P())
    return jax.shard_map(local, mesh=mesh, in_specs=in_specs, out_specs=out_specs, check_vma=False)
```

```python
import functools

import jax
import jax.numpy as jnp
from jax import lax
from jax.experimental import pallas as pl
from jax.experimental.pallas import tpu as pltpu
from jax.sharding import PartitionSpec as P

mix_rate = 0.5
MESH = pl.DeviceIdType.MESH
PIECES = 4
STRIPS = 1
SIDE = 2


def gather_kernel(
    rows,
    model,
    *refs,
):
    sources, (og, ou, od, norm), refs = refs[:11], refs[11:15], refs[15:]
    held, refs = refs[:11], refs[11:]
    wg, lg, hg, wu, lu, hu, wd, ld, hd, nt, ns = held
    fetch_sem, link_send, link_recv, pair_send, pair_recv, norm_send, norm_recv = refs
    me = lax.axis_index("rows")
    depth = lax.axis_index("model")
    core = lax.rem(me, 2)
    x = lax.rem(me // 2, SIDE)
    y = me // (2 * SIDE)

    def device(y, x, core):
        return (y * SIDE + x) * 2 + core

    pair = device(y, x, 1 - core)
    near_x = device(y, 1 - x, core)
    near_y = device(1 - y, x, core)
    far = device(1 - y, 1 - x, core)

    def shifted(position, size, step):
        return lax.rem(position + step, size)

    barrier = pltpu.get_barrier_semaphore()
    for step in range(1, rows):
        pl.semaphore_signal(barrier, inc=1, device_id={"rows": shifted(me, rows, step)}, device_id_type=MESH)
    for step in range(1, model):
        pl.semaphore_signal(barrier, inc=1, device_id={"model": shifted(depth, model, step)}, device_id_type=MESH)

    outs = (og, ou, od)
    fetches = {}

    def fetch(key, i, *cut):
        fetches[key] = pltpu.make_async_copy(
            sources[i].at[cut] if cut else sources[i], held[i].at[cut] if cut else held[i],
            fetch_sem.at[len(fetches)],
        )

    long = wg.shape[1] // PIECES
    long_down = wd.shape[0] // PIECES
    short = wg.shape[0]
    short_down = wd.shape[1]
    units = [(a, k) for k in range(PIECES) for a in range(3)]

    for u, (a, k) in enumerate(units):
        if k == 0:
            fetch(("low", a), 3 * a + 1)
            fetch(("high", a), 3 * a + 2)
        if a < 2:
            fetch(u, 3 * a, pl.ds(0, short), pl.ds(k * long, long))
        else:
            fetch(u, 3 * a, pl.ds(k * long_down, long_down), pl.ds(0, short_down))
    fetch("train", 9)
    fetch("step", 10)
    for f in fetches.values():
        f.start()

    def place(u, owner):
        a, k = units[u]
        if a < 2:
            return outs[a].at[pl.ds(k * long, long), pl.ds(pl.multiple_of(owner * short, short), short)]
        return outs[a].at[pl.ds(pl.multiple_of(owner * short_down, short_down), short_down), pl.ds(k * long_down, long_down)]

    def compute(u):
        a, k = units[u]
        if k == 0:
            fetches["low", a].wait()
            fetches["high", a].wait()
        fetches[u].wait()
        if a < 2:
            w, low, high = ((wg, lg, hg), (wu, lu, hu))[a]
            cut = slice(k * long, (k + 1) * long)
            weight, low, high = w[:, cut], low[...], high[:, cut]
        else:
            cut = slice(k * long_down, (k + 1) * long_down)
            weight, low, high = wd[cut, :], ld[:, cut], hd[...]
        merged = weight.astype(jnp.float32) + mix_rate * lax.dot_general(
            low, high, (((0,), (0,)), ((), ())), preferred_element_type=jnp.float32
        )
        place(u, me)[...] = merged.astype(jnp.bfloat16).T

    def copy(u, owner, send, recv, target):
        return pltpu.make_async_remote_copy(
            src_ref=place(u, owner), dst_ref=place(u, owner), send_sem=send, recv_sem=recv,
            device_id={"rows": target}, device_id_type=MESH,
        )

    def link(lane, u, owner, target):
        return copy(u, owner, link_send.at[lane, u], link_recv.at[lane, u], target)

    def across(lane, u, owner):
        return copy(u, owner, pair_send.at[lane, u], pair_recv.at[lane, u], pair)

    def send_own(u):
        link(0, u, me, near_x).start()
        link(1, u, me, near_y).start()
        across(3, u, me).start()

    count = len(units)
    compute(0)
    fetches["train"].wait()
    fetches["step"].wait()
    norm[me, depth] = jnp.zeros(norm.shape[2:], norm.dtype)
    norm[me, depth, :, : nt.shape[1]] = nt[...] + ns[...]
    pl.semaphore_wait(barrier, rows - 1 + model - 1)
    for u in range(1, count):
        compute(u)
        send_own(u - 1)

    def norm_copy(step, send):
        if step < model:
            to = {"model": shifted(depth, model, step)}
            ref = norm.at[me, depth] if send else norm.at[me, shifted(depth, model, model - step)]
            slot = step - 1
        else:
            step = step - model + 1
            to = {"rows": shifted(me, rows, step)}
            ref = norm.at[me] if send else norm.at[shifted(me, rows, rows - step)]
            slot = model - 1 + step - 1
        return pltpu.make_async_remote_copy(
            src_ref=ref, dst_ref=ref, send_sem=norm_send.at[slot], recv_sem=norm_recv.at[slot],
            device_id=to, device_id_type=MESH,
        )

    for step in range(1, model):
        norm_copy(step, True).start()
    send_own(count - 1)
    for step in range(1, model):
        norm_copy(step, False).wait_recv()
    for step in range(model, model + rows - 1):
        norm_copy(step, True).start()

    for u in range(count):
        link(0, u, near_x, near_x).wait_recv()
        if u % 2 == 0:
            link(2, u, near_x, near_y).start()
        across(0, u, near_x).start()
        link(1, u, near_y, near_y).wait_recv()
        if u % 2 == 1:
            link(2, u, near_y, near_x).start()
        across(1, u, near_y).start()
    for u in range(count):
        link(2, u, far, near_x).wait_recv()
        across(2, u, far).start()

    for step in range(model, model + rows - 1):
        norm_copy(step, False).wait_recv()
    for step in range(1, model + rows - 1):
        norm_copy(step, True).wait_send()
    pair_x, pair_y = device(y, 1 - x, 1 - core), device(1 - y, x, 1 - core)
    pair_far = device(1 - y, 1 - x, 1 - core)
    for u in range(count):
        link(0, u, me, near_x).wait_send()
        link(1, u, me, near_y).wait_send()
        link(2, u, near_x if u % 2 == 0 else near_y, near_x).wait_send()
        for lane, mine, theirs in ((3, me, pair), (0, near_x, pair_x), (1, near_y, pair_y), (2, far, pair_far)):
            across(lane, u, mine).wait_send()
            across(lane, u, theirs).wait_recv()


def gathered(rows, model, arrays):
    weight_gate, weight_up, weight_down, norm_train = arrays[0], arrays[3], arrays[6], arrays[9]
    shapes = [
        (weight_gate.shape[1], weight_gate.shape[0] * rows),
        (weight_up.shape[1], weight_up.shape[0] * rows),
        (weight_down.shape[1] * rows, weight_down.shape[0]),
    ]
    lanes = -(-norm_train.shape[1] // 128) * 128
    count = 3 * PIECES
    small = rows - 1 + model - 1
    dma = pltpu.SemaphoreType.DMA
    vmem = pl.BlockSpec(memory_space=pltpu.VMEM)
    return pl.pallas_call(
        functools.partial(gather_kernel, rows, model),
        out_shape=[pltpu.VMEM(s, jnp.bfloat16) for s in shapes] + [pltpu.VMEM((rows, model, 1, lanes), jnp.float32)],
        in_specs=[pl.BlockSpec(memory_space=pltpu.HBM)] * len(arrays),
        out_specs=[vmem] * 4,
        scratch_shapes=[pltpu.VMEM(a.shape, a.dtype) for a in arrays]
        + [
            dma((count + 8,)),
            dma((3, count)), dma((3, count)), dma((4, count)), dma((4, count)), dma((small,)), dma((small,)),
        ],
        compiler_params=pltpu.CompilerParams(collective_id=0, has_side_effects=True, vmem_limit_bytes=39 * 2**20 + 5 * 2**17),
    )(*arrays)


def write_kernel(size, lanes, g, u, d, norm, og, ou, od, out, sems):
    strip = g.shape[0] // STRIPS
    copies = [
        pltpu.make_async_copy(s.at[pl.ds(k * strip, strip)], t.at[pl.ds(k * strip, strip)], sems.at[i, k])
        for k in range(STRIPS)
        for i, (s, t) in enumerate(((g, og), (u, ou), (d, od)))
    ]
    for c in copies:
        c.start()
    rows, model = norm.shape[:2]
    parts = [norm[r, m][:, :size] for r in range(rows) for m in range(model)]
    group = lanes // size
    packed = [jnp.concatenate(parts[i : i + group], axis=1) for i in range(0, len(parts), group)]
    out[...] = jnp.concatenate(packed, axis=0).astype(out.dtype)
    for c in copies:
        c.wait()


def written(size, arrays):
    lanes = arrays[3].shape[3]
    total = arrays[3].shape[0] * arrays[3].shape[1] * size
    hbm, vmem = pl.BlockSpec(memory_space=pltpu.HBM), pl.BlockSpec(memory_space=pltpu.VMEM)
    return pl.pallas_call(
        functools.partial(write_kernel, size, lanes),
        out_shape=[jax.ShapeDtypeStruct(a.shape, a.dtype) for a in arrays[:3]]
        + [jax.ShapeDtypeStruct((total // lanes, lanes), jnp.bfloat16)],
        in_specs=[vmem] * 4,
        out_specs=[hbm] * 3 + [vmem],
        scratch_shapes=[pltpu.SemaphoreType.DMA((3, STRIPS))],
        compiler_params=pltpu.CompilerParams(vmem_limit_bytes=2**20),
    )(*arrays)


def local_kernel(rows, model, *arrays):
    arrays = tuple(a.T if i in (1, 4, 7) else a for i, a in enumerate(arrays[:9])) + tuple(
        a.reshape(1, -1) for a in arrays[9:]
    )
    gate, up, down, norm = gathered(rows, model, arrays)
    gate, up, down, serve_norm = written(arrays[9].shape[1], (gate, up, down, norm))
    return gate, up, down, serve_norm.reshape(-1)


def merge(weight, low, high):
    full = weight.astype(jnp.float32) + mix_rate * jnp.dot(low, high, preferred_element_type=jnp.float32)
    return full.astype(jnp.bfloat16).T


def local_plain(*arrays):
    gate, up, down = merge(*arrays[:3]), merge(*arrays[3:6]), merge(*arrays[6:9])
    return (
        lax.all_gather(gate, "rows", axis=1, tiled=True),
        lax.all_gather(up, "rows", axis=1, tiled=True),
        lax.all_gather(down, "rows", axis=0, tiled=True),
        lax.all_gather((arrays[9] + arrays[10]).astype(jnp.bfloat16), ("rows", "model"), axis=0, tiled=True),
    )


def solution(mesh):
    rows, model = mesh.shape["rows"], mesh.shape["model"]
    local = functools.partial(local_kernel, rows, model) if rows == 2 * SIDE * SIDE else local_plain
    in_specs = (
        P("rows", "model"), P("rows", None), P(None, "model"),
        P("rows", "model"), P("rows", None), P(None, "model"),
        P("model", "rows"), P("model", None), P(None, "rows"),
        P(("rows", "model")), P(("rows", "model")),
    )
    out_specs = (P("model", None), P("model", None), P(None, "model"), P())
    return jax.shard_map(local, mesh=mesh, in_specs=in_specs, out_specs=out_specs, check_vma=False)
```
